512 devices in a mesh: rows: 128 (over z, y, core), trees: 4 (over x).
Axes of the slice: x: 4, y: 8, z: 8, core: 2. Of those that a mesh axis runs over, the one named last changes fastest.
Arguments:
- node_of_row: int32 [4, 262144], P('trees', 'rows'), may hold values from 0 to 63
- bag_weight: int32 [4, 262144], P('trees', 'rows'), may hold values from 0 to 6, as said below
- smaller_side: int32 [4, 32], P('trees'), may hold values from 0 to 1
- bins: int32 [262144, 256], P('rows'), may hold values from 0 to 31
- target: float32 [262144], P('rows'), may hold values from -6 to 6
- parent_hist: float32 [4, 256, 3072], P('trees', 'rows')
Outputs:
- child_hist: float32 [4, 256, 6144], P('trees', 'rows')
- best_gain: float32 [4, 64], P('trees')
- importance: float32 [256], P('rows')
The draws below stay inside these ranges and needn't reach their ends.
Inputs may be any that keep to these rules, and one draw needn't show every extreme that they name: `bag_weight`: poisson weights with mean one.
All inputs are finite; a program needn't handle non-finite values.
Results may differ from the reference program's by a relative error of at most 0.002.
Values sent between devices are 32-bit elements; how exact they have to be, the bound alone decides.
A program may use at most 64 MiB of HBM per device.

```python
import math
import jax
import jax.numpy as jnp
import numpy as np
from jax import lax

FEAT = 256
BINS = 32
PAIRS = 32
ROWS = 262144
TREES = 4


def draw_bag_weight(key, part):
    drawn = jax.random.randint(jax.random.fold_in(key, 11), (TREES, ROWS), 0, 1 << 20)
    limits = jnp.array([385749, 771499, 964396, 1028631, 1044680, 1047956], jnp.int32)
    return jnp.sum((drawn[..., None] >= limits).astype(jnp.int32), axis=-1).astype(jnp.int32)


def draw_parent_hist(key, part):
    first, second, third = jax.random.split(jax.random.fold_in(key, 23), 3)
    shape = (TREES, FEAT, BINS, PAIRS)
    middle = ROWS / (2.0 * PAIRS * BINS)
    counts = middle * jax.random.uniform(first, shape, jnp.float32, 0.3, 2.5)
    sums = jax.random.normal(second, shape, jnp.float32) * jnp.sqrt(middle + 1.0)
    squares = counts * jax.random.uniform(third, shape, jnp.float32, 0.5, 2.0)
    stacked = jnp.stack([counts, sums, squares], axis=-1)
    return stacked.reshape(TREES, FEAT, BINS * PAIRS * 3).astype(jnp.float32)


def touch_ends(values, rng, low, high):
    spot = [jax.random.randint(jax.random.fold_in(rng, axis), (), 0, length) for axis, length in enumerate(values.shape)]
    widest = values.shape.index(max(values.shape))
    beside = spot[:widest] + [(spot[widest] + 1) % values.shape[widest]] + spot[widest + 1:]
    return values.at[tuple(spot)].set(low).at[tuple(beside)].set(high)


def shard_levels(stream_key, shape, pieces, low, largest):
    loudness, own = 1.0, jax.random.fold_in(stream_key, 6)
    for axis_at, blocks in pieces:
        draws = jnp.exp(jax.random.uniform(jax.random.fold_in(own, axis_at), (blocks,), jnp.float32, low / len(pieces), largest / len(pieces)))
        loudness = loudness * jnp.repeat(draws, shape[axis_at] // blocks).reshape([-1 if axis == axis_at else 1 for axis in range(len(shape))])
    return loudness


def rank_bounds(number_of, lean):
    portions = [(1 << 20) // math.isqrt(rank ** lean) + 1 for rank in range(1, number_of + 1)]
    scale = 1 + sum(portions) // (1 << 30)
    return np.cumsum(np.array([max(1, weight // scale) for weight in portions]))


def skewed_ids(rng, extent, number_of, lean):
    listing = rank_bounds(number_of, lean)
    lot = jax.random.randint(jax.random.fold_in(rng, 1), extent, 0, int(listing[number_of - 1]))
    standing = jnp.searchsorted(jnp.asarray(listing, jnp.int32), lot, side="right")
    return jax.random.permutation(jax.random.fold_in(rng, 2), number_of)[standing].astype(jnp.int32)


def scatter_about(key, shape, spread, most, cuts=(), held_as=jnp.bfloat16):
    level = shard_levels(key, shape, cuts, -0.22, 0.18) if cuts else 1.0
    values = jax.random.normal(key, shape, jnp.float32) * spread * level
    return jnp.minimum(jnp.maximum(values, -most), most).astype(held_as)


def setup_inputs(seed: int = 0) -> dict:
    splits = jax.random.split(jax.random.key(seed), 7)
    return {
        "node_of_row": touch_ends(skewed_ids(splits[0], (TREES, ROWS), 2 * PAIRS, 2), jax.random.fold_in(splits[0], 3), 0, (2 * PAIRS) - 1).astype(jnp.int32),
        "bag_weight": draw_bag_weight(jax.random.fold_in(splits[6], 71), 0),
        "smaller_side": touch_ends(jax.random.randint(splits[2], (TREES, PAIRS), 0, 2), jax.random.fold_in(splits[2], 1), 0, 1).astype(jnp.int32),
        "bins": touch_ends(jax.random.randint(splits[3], (ROWS, FEAT), 0, BINS), jax.random.fold_in(splits[3], 1), 0, BINS - 1).astype(jnp.int32),
        "target": scatter_about(splits[4], (ROWS,), 1.0, 6.0, ((0, 128),), jnp.float32),
        "parent_hist": draw_parent_hist(jax.random.fold_in(splits[6], 71), 0),
    }


def tree_small(nodes, weights, flags, bins, target):
    pair = nodes // 2
    side = nodes % 2
    keep = (side == flags[pair]).astype(jnp.float32)
    wk = weights.astype(jnp.float32) * keep
    stats = jnp.stack([wk, wk * target, wk * target * target], axis=1).astype(jnp.bfloat16).astype(jnp.float32)
    width = min(FEAT, 32)

    def block(index):
        cols = lax.dynamic_slice_in_dim(bins, (index * width).astype(jnp.int32), width, 1)
        fidx = jnp.arange(width, dtype=jnp.int32)
        ids = (fidx[None, :] * BINS + cols) * PAIRS + pair[:, None]
        data = jnp.broadcast_to(stats[:, None, :], (stats.shape[0], width, 3))
        summed = jax.ops.segment_sum(data.reshape(-1, 3), ids.reshape(-1), num_segments=width * BINS * PAIRS)
        return summed.reshape(width, BINS, PAIRS, 3)

    blocks = lax.map(block, jnp.arange(FEAT // width, dtype=jnp.int32))
    return blocks.reshape(FEAT, BINS, PAIRS, 3)


def gains_of(children):
    count = children[..., 0]
    total = children[..., 1]
    ccum = jnp.cumsum(count, axis=1)
    scum = jnp.cumsum(total, axis=1)
    call = ccum[:, -1:, :]
    sall = scum[:, -1:, :]
    left_c = ccum[:, :-1, :]
    left_s = scum[:, :-1, :]
    gain = left_s * left_s / (jnp.maximum(left_c, 0.0) + 1.0)
    gain = gain + (sall - left_s) ** 2 / (jnp.maximum(call - left_c, 0.0) + 1.0)
    gain = gain - sall * sall / (jnp.maximum(call, 0.0) + 1.0)
    return jnp.max(gain, axis=1)


def reference(node_of_row, bag_weight, smaller_side, bins, target, parent_hist):
    hists = []
    bests = []
    featsum = jnp.zeros((FEAT,), jnp.float32)
    for tree in range(TREES):
        small = tree_small(node_of_row[tree], bag_weight[tree], smaller_side[tree], bins, target)
        parent = parent_hist[tree].reshape(FEAT, BINS, PAIRS, 3)
        sibling = parent - small
        take = (jnp.arange(2, dtype=jnp.int32)[None, :] == smaller_side[tree][:, None])
        children = jnp.where(take[None, None, :, :, None], small[:, :, :, None, :], sibling[:, :, :, None, :])
        children = children.reshape(FEAT, BINS, 2 * PAIRS, 3)
        hists.append(children.reshape(FEAT, BINS * 2 * PAIRS * 3))
        fgain = gains_of(children)
        bests.append(jnp.max(fgain, axis=0))
        featsum = featsum + jnp.sum(fgain, axis=1)
    importance = featsum / (TREES * 2 * PAIRS)
    return jnp.stack(hists), jnp.stack(bests), importance
```

```python
import functools

import jax
import jax.numpy as jnp
from jax import lax
from jax.experimental import pallas as pl
from jax.experimental.pallas import tpu as pltpu
from jax.sharding import Mesh
from jax.sharding import PartitionSpec as P

ROWS = ("rows_0", "rows_1", "rows_2")
MESH = pl.DeviceIdType.MESH
HIGHEST = lax.Precision.HIGHEST
f32 = jnp.float32
bf16 = jnp.bfloat16
i32 = jnp.int32

ORDER = (4, 3, -3, 2, -2, 1, -1, 0)
SLOT = {delta: i for i, delta in enumerate(ORDER)}
NR = 2048
LOW = -3.0e38


def iota(shape, dim):
    return lax.broadcasted_iota(i32, shape, dim)


def kernel(
    node_h, bag_h, flag_h, bins_h, tgt_h, par_h,
    child_o, best_o, imp_o,
    node_v, bag_v, flag_v, bins_v, tgt_v, par_v,
    bins_b, ev, spread, own, peer, core_r, ring_r, turned, quad_r,
    p16, pchild, amat,
    best_s, best_ra, best_t, best_rb, imp_s, imp_r,
    in_sem, core_ss, core_rs, ring_ss, ring_rs, quad_ss, quad_rs,
    ba_ss, ba_rs, bb_ss, bb_rs, im_ss, im_rs,
):
    z = lax.axis_index("rows_0")
    y = lax.axis_index("rows_1")
    c = lax.axis_index("rows_2")
    t = lax.axis_index("trees")

    def wrap(v, n):
        return lax.rem(v + n, n)

    def along_y(off, oc=0):
        return (z, lax.rem(y + off, 8), lax.rem(c + oc, 2), t)

    def along_z(off):
        return (lax.rem(z + off, 8), y, c, t)

    def along_x(off):
        return (z, y, c, lax.rem(t + off, 4))

    def along_p(off):
        off = off % 8
        return (lax.rem(z + off * c, 8), lax.rem(y + off * (1 - c), 8), c, t)

    def along_q(off):
        return (lax.rem(z + off * (1 - c), 8), lax.rem(y + off * c, 8), c, t)

    loads = []
    for i in range(8):
        cp = pltpu.make_async_copy(
            bins_h.at[pl.ds(256 * i, 256)], bins_v.at[pl.ds(256 * i, 256)], in_sem.at[i]
        )
        cp.start()
        loads.append(cp)
    small = []
    for i, (src, dst) in enumerate(
        ((node_h, node_v), (bag_h, bag_v), (flag_h, flag_v), (tgt_h, tgt_v), (par_h, par_v))
    ):
        cp = pltpu.make_async_copy(src, dst, in_sem.at[8 + i])
        cp.start()
        small.append(cp)

    barrier = pltpu.get_barrier_semaphore()
    greeted = 0
    for oy in range(8):
        for oc in range(2):
            if oy or oc:
                pl.semaphore_signal(barrier, inc=1, device_id=along_y(oy, oc), device_id_type=MESH)
                greeted += 1
    for off in range(1, 8):
        pl.semaphore_signal(barrier, inc=1, device_id=along_z(off), device_id_type=MESH)
        greeted += 1
    for off in range(1, 4):
        pl.semaphore_signal(barrier, inc=1, device_id=along_x(off), device_id_type=MESH)
        greeted += 1

    for cp in small:
        cp.wait()
    flags = flag_v[...]
    row96 = iota((96, 1), 0)
    pair96 = lax.div(row96, 3)
    stat96 = row96 - 3 * pair96
    flag96 = jnp.sum(
        jnp.where(iota((96, 32), 1) == lax.div(iota((96, 32), 0), 3), flags, 0), axis=1, keepdims=True
    )
    chosen = 2 * pair96 + flag96
    for i in range(4):
        part = pl.ds(512 * i, 512)
        node = node_v[:, part]
        wk = bag_v[:, part].astype(f32)
        tgt = tgt_v[:, part]
        first = wk * tgt
        second = first * tgt
        stat = jnp.where(stat96 == 0, wk, jnp.where(stat96 == 1, first, second))
        spread[:, part] = jnp.where(node == chosen, stat, 0.0).astype(bf16)

    for i in range(8):
        loads[i].wait()
        part = pl.ds(256 * i, 256)
        bins_b[part, :] = bins_v[part, :].astype(bf16)

    lane256 = iota((1, 256), 1)
    lane_dd = lax.div(lane256, 128)
    lane_q = lax.rem(lax.div(lane256, 16), 8)
    lane_k = lax.rem(lax.div(lane256, 8), 2)
    lane_b = (4 * lax.rem(lane256, 8)).astype(f32)

    def tile(pair_i, h, dst):
        pos = y * (1 - h) + z * h
        d0 = wrap(pos + ORDER[2 * pair_i], 8)
        d1 = wrap(pos + ORDER[2 * pair_i + 1], 8)
        d = d0 + (d1 - d0) * lane_dd
        source = lane_q * (32 - 28 * h) + d * (4 + 28 * h) + 2 * h + lane_k
        expand = jnp.where(iota((256, 256), 0) == source, 1.0, 0.0).astype(bf16)

        def widen(i, carry):
            part = pl.ds(pl.multiple_of(512 * i, 512), 512)
            ev[part, :] = jnp.dot(bins_b[part, :], expand, preferred_element_type=f32).astype(bf16)
            return carry

        lax.fori_loop(0, 4, widen, 0)

        def one(bh, carry):
            level = (lane_b + bh.astype(f32)).astype(bf16)
            acc = None
            for i in range(8):
                part = slice(256 * i, 256 * i + 256)
                hot = jnp.where(ev[part, :] == level, jnp.ones((), bf16), jnp.zeros((), bf16))
                term = jnp.dot(spread[:, part], hot, preferred_element_type=f32)
                acc = term if acc is None else acc + term
            at = pl.ds(pl.multiple_of(96 * bh, 96), 96)
            dst[2 * pair_i, at, :] = acc[:, :128]
            dst[2 * pair_i + 1, at, :] = acc[:, 128:]
            return carry

        lax.fori_loop(0, 4, one, 0)

    def core_copy(slot):
        return pltpu.make_async_remote_copy(
            src_ref=peer.at[slot], dst_ref=core_r.at[slot],
            send_sem=core_ss.at[slot], recv_sem=core_rs.at[slot],
            device_id=(z, y, 1 - c, t), device_id_type=MESH,
        )

    def ring_copy(way, step, half):
        delta = (4 - step) * (1 if way == 0 else -1)
        slot = SLOT[4 if step == 0 else delta]
        rows = pl.ds(192 * half, 192)
        return pltpu.make_async_remote_copy(
            src_ref=own.at[slot, rows], dst_ref=ring_r.at[way, step, rows],
            send_sem=ring_ss.at[way, step, half], recv_sem=ring_rs.at[way, step, half],
            device_id=along_p(1 if way == 0 else -1), device_id_type=MESH,
        )

    def halves(way, step):
        return (way,) if step == 0 else (0, 1)

    def merge_core(slot):
        core_copy(slot).wait_recv()
        own[slot] += core_r[slot]

    def step_sends(step):
        for half in (0, 1):
            for way in (0, 1):
                delta = (4 - step) * (1 if way == 0 else -1)
                slot = SLOT[delta]
                rows = pl.ds(192 * half, 192)
                if half in halves(way, step - 1):
                    ring_copy(way, step - 1, half).wait_recv()
                    own[slot, rows, :] += ring_r[way, step - 1, rows, :]
                ring_copy(way, step, half).start()

    for pair_i in range(4):
        tile(pair_i, 1 - c, peer)
        if pair_i == 0:
            pl.semaphore_wait(barrier, greeted)
        core_copy(2 * pair_i).start()
        core_copy(2 * pair_i + 1).start()
        tile(pair_i, c, own)
        merge_core(2 * pair_i)
        merge_core(2 * pair_i + 1)
        if pair_i == 0:
            ring_copy(0, 0, 0).start()
            ring_copy(1, 0, 1).start()
        else:
            step_sends(pair_i)

    flag384 = jnp.concatenate([flag96] * 4, axis=0)
    out_lane = iota((1, 768), 1)
    out_bh = lax.div(out_lane, 192)
    out_rest = out_lane - 192 * out_bh
    out_pair = lax.div(out_rest, 6)
    out_six = out_rest - 6 * out_pair
    out_child = lax.div(out_six, 3)
    out_from = 96 * out_bh + 3 * out_pair + (out_six - 3 * out_child)
    for k in range(2):
        for bl in range(8):
            p16[8 * k + bl : 8 * k + bl + 1, :] = par_v[0, k : k + 1, 384 * bl : 384 * bl + 384]
    match = iota((384, 768), 0) == out_from
    is_small = flag384 == out_child
    amat[...] = jnp.where(match, jnp.where(is_small, 1.0, -1.0), 0.0)
    bmat = jnp.where(match, jnp.where(is_small, 0.0, 1.0), 0.0)
    parent = p16[...]
    pchild[...] = jnp.dot(parent, bmat, preferred_element_type=f32, precision=HIGHEST)

    lane = iota((16, 384), 1)
    sub = lax.rem(iota((16, 384), 0), 8)

    def cumulative(x):
        x1 = x + jnp.where(lane >= 96, pltpu.roll(x, 96, 1), 0.0)
        x2 = x1 + jnp.where(lane >= 192, pltpu.roll(x1, 192, 1), 0.0)
        t3 = jnp.where(lane >= 288, x2, 0.0)
        t4 = t3 + pltpu.roll(t3, 96, 1)
        tot = t4 + pltpu.roll(t4, 192, 1)
        before = jnp.where(sub >= 1, pltpu.roll(tot, 1, 0), 0.0)
        for s in (1, 2, 4):
            before = before + jnp.where(sub >= s, pltpu.roll(before, s, 0), 0.0)
        whole = jnp.sum(tot.reshape(2, 8, 384), axis=1, keepdims=True)
        whole = jnp.broadcast_to(whole, (2, 8, 384)).reshape(16, 384)
        return x2 + before, whole

    def gain_of(cb, sb, call, sall):
        gain = sb * sb / (jnp.maximum(cb, 0.0) + 1.0)
        rest = sall - sb
        gain = gain + rest * rest / (jnp.maximum(call - cb, 0.0) + 1.0)
        gain = gain - sall * sall / (jnp.maximum(call, 0.0) + 1.0)
        gain = jnp.where((sub == 7) & (lane >= 288), LOW, gain)
        top = jnp.max(gain.reshape(2, 8, 384), axis=1, keepdims=True)
        top = jnp.broadcast_to(top, (2, 8, 384)).reshape(16, 384)
        top = jnp.maximum(top, pltpu.roll(top, 192, 1))
        return jnp.maximum(top, pltpu.roll(top, 96, 1))

    def left_one(x):
        return pltpu.roll(x, 383, 1)

    pcum, pall = cumulative(parent)
    psum, psall = left_one(pcum), left_one(pall)

    last = SLOT[0]
    total = own[last]
    for half in (0, 1):
        for way in (0, 1):
            ring_copy(way, 3, half).wait_recv()
    total = total + ring_r[0, 3] + ring_r[1, 3]
    turned[...] = total.T

    qpos = z * (1 - c) + y * c

    def quad_copy(off):
        to = lax.rem(qpos + off, 8)
        return pltpu.make_async_remote_copy(
            src_ref=turned.at[pl.ds(pl.multiple_of(16 * to, 16), 16)], dst_ref=quad_r.at[off],
            send_sem=quad_ss.at[off], recv_sem=quad_rs.at[off],
            device_id=along_q(off), device_id_type=MESH,
        )

    far_first = (4, 3, 5, 2, 6, 1, 7)
    for off in far_first:
        quad_copy(off).start()
    hist = turned[pl.ds(pl.multiple_of(16 * qpos, 16), 16), :]
    for off in (1, 7, 2, 6, 3, 5, 4):
        quad_copy(off).wait_recv()
        hist = hist + quad_r[off]

    scum, sall = cumulative(hist)
    ssum, ssall = left_one(scum), left_one(sall)
    gain_s = gain_of(scum, ssum, sall, ssall)
    gain_b = gain_of(pcum - scum, psum - ssum, pall - sall, psall - ssall)
    third = lax.rem(lane, 3)
    both = jnp.where((lane < 96) & (third == 0), gain_s + gain_b, 0.0)
    feat = jnp.sum(both, axis=1, keepdims=True)
    lane8 = iota((8, 128), 1)
    imp_s[...] = jnp.where(lane8 == 0, feat[0:8], jnp.where(lane8 == 1, feat[8:16], 0.0))
    top_s = jnp.maximum(gain_s[0:8], gain_s[8:16])
    top_b = jnp.maximum(gain_b[0:8], gain_b[8:16])
    mixed = jnp.where(third[0:8] == 0, top_s, pltpu.roll(top_b, 1, 1))
    best_s[...] = mixed[:, :128]

    def best_a(oy, oc):
        slot = 2 * oy + oc
        return pltpu.make_async_remote_copy(
            src_ref=best_s, dst_ref=best_ra.at[slot],
            send_sem=ba_ss.at[slot], recv_sem=ba_rs.at[slot],
            device_id=along_y(oy, oc), device_id_type=MESH,
        )

    def best_b(off):
        return pltpu.make_async_remote_copy(
            src_ref=best_t, dst_ref=best_rb.at[off],
            send_sem=bb_ss.at[off], recv_sem=bb_rs.at[off],
            device_id=along_z(off), device_id_type=MESH,
        )

    def imp_copy(off):
        return pltpu.make_async_remote_copy(
            src_ref=imp_s, dst_ref=imp_r.at[off],
            send_sem=im_ss.at[off], recv_sem=im_rs.at[off],
            device_id=along_x(off), device_id_type=MESH,
        )

    others = [(oy, oc) for oy in (4, 3, 5, 2, 6, 1, 7, 0) for oc in (0, 1) if oy or oc]
    for oy, oc in others:
        best_a(oy, oc).start()
    for off in (2, 1, 3):
        imp_copy(off).start()

    kids = pchild[...] + jnp.dot(hist, amat[...], preferred_element_type=f32, precision=HIGHEST)
    for k in range(2):
        for bl in range(8):
            child_o[0, k : k + 1, 768 * bl : 768 * bl + 768] = kids[8 * k + bl : 8 * k + bl + 1, :]

    top = best_s[...]
    for oy, oc in others:
        best_a(oy, oc).wait_recv()
        top = jnp.maximum(top, best_ra[2 * oy + oc])
    best_t[...] = top
    for off in far_first:
        best_b(off).start()

    flag_col = jnp.sum(jnp.where(iota((32, 32), 0) == iota((32, 32), 1), flags, 0), axis=1, keepdims=True)
    node_lane = iota((32, 64), 1)
    node_flag = jnp.sum(
        jnp.where(lax.div(node_lane, 2) == iota((32, 64), 0), flag_col, 0), axis=0, keepdims=True
    )
    q_lane = iota((1, 64), 1)
    q_pair = lax.div(q_lane, 2)
    taken = 3 * q_pair + jnp.where(q_lane - 2 * q_pair == node_flag, 0, 1)
    pick = jnp.where(iota((128, 64), 0) == taken, 1.0, 0.0)

    share = imp_s[...]
    for off in (1, 3, 2):
        imp_copy(off).wait_recv()
        share = share + imp_r[off]
    imp_o[...] = share[0:1, 0:2] * (1.0 / 256.0)

    for off in far_first:
        best_b(off).wait_recv()
        top = jnp.maximum(top, best_rb[off])
    best_o[...] = jnp.dot(top, pick, preferred_element_type=f32, precision=HIGHEST)[0:1, :]

    for slot in range(8):
        core_copy(slot).wait_send()
    for way in (0, 1):
        for step in range(4):
            for half in halves(way, step):
                ring_copy(way, step, half).wait_send()
    for off in range(1, 8):
        quad_copy(off).wait_send()
        best_b(off).wait_send()
    for oy, oc in others:
        best_a(oy, oc).wait_send()
    for off in range(1, 4):
        imp_copy(off).wait_send()


def shards(node_of_row, bag_weight, smaller_side, bins, target, parent_hist):
    any_space = pl.BlockSpec(memory_space=pl.ANY)
    vmem = pl.BlockSpec(memory_space=pltpu.VMEM)
    dma = pltpu.SemaphoreType.DMA
    child, best, imp = pl.pallas_call(
        kernel,
        out_shape=(
            jax.ShapeDtypeStruct((1, 2, 6144), f32),
            jax.ShapeDtypeStruct((1, 64), f32),
            jax.ShapeDtypeStruct((1, 2), f32),
        ),
        in_specs=[any_space] * 6,
        out_specs=(vmem, vmem, vmem),
        scratch_shapes=[
            pltpu.VMEM((1, NR), i32),
            pltpu.VMEM((1, NR), i32),
            pltpu.VMEM((1, 32), i32),
            pltpu.VMEM((NR, 256), i32),
            pltpu.VMEM((1, NR), f32),
            pltpu.VMEM((1, 2, 3072), f32),
            pltpu.VMEM((NR, 256), bf16),
            pltpu.VMEM((NR, 256), bf16),
            pltpu.VMEM((96, NR), bf16),
            pltpu.VMEM((8, 384, 128), f32),
            pltpu.VMEM((8, 384, 128), f32),
            pltpu.VMEM((8, 384, 128), f32),
            pltpu.VMEM((2, 4, 384, 128), f32),
            pltpu.VMEM((128, 384), f32),
            pltpu.VMEM((8, 16, 384), f32),
            pltpu.VMEM((16, 384), f32),
            pltpu.VMEM((16, 768), f32),
            pltpu.VMEM((384, 768), f32),
            pltpu.VMEM((8, 128), f32),
            pltpu.VMEM((16, 8, 128), f32),
            pltpu.VMEM((8, 128), f32),
            pltpu.VMEM((8, 8, 128), f32),
            pltpu.VMEM((8, 128), f32),
            pltpu.VMEM((4, 8, 128), f32),
            dma((13,)),
            dma((8,)), dma((8,)),
            dma((2, 4, 2)), dma((2, 4, 2)),
            dma((8,)), dma((8,)),
            dma((16,)), dma((16,)),
            dma((8,)), dma((8,)),
            dma((4,)), dma((4,)),
        ],
        compiler_params=pltpu.CompilerParams(
            collective_id=0, has_side_effects=True, vmem_limit_bytes=40 * 1024 * 1024
        ),
    )(node_of_row, bag_weight, smaller_side, bins, target.reshape(1, NR), parent_hist)
    return child, best, imp.reshape(2)


def solution(mesh):
    finer = Mesh(
        mesh.devices.reshape(8, 8, 2, mesh.shape["trees"]), ("rows_0", "rows_1", "rows_2", "trees")
    )
    return jax.shard_map(
        shards,
        mesh=finer,
        in_specs=(
            P("trees", ROWS),
            P("trees", ROWS),
            P("trees", None),
            P(ROWS, None),
            P(ROWS),
            P("trees", ROWS, None),
        ),
        out_specs=(P("trees", ROWS, None), P("trees", None), P(ROWS)),
        check_vma=False,
    )
```

```python
import functools

import jax
import jax.numpy as jnp
from jax import lax
from jax.experimental import pallas as pl
from jax.experimental.pallas import tpu as pltpu
from jax.sharding import Mesh
from jax.sharding import PartitionSpec as P

ROWS = ("rows_0", "rows_1", "rows_2")
MESH = pl.DeviceIdType.MESH
HIGHEST = lax.Precision.HIGHEST
f32 = jnp.float32
bf16 = jnp.bfloat16
i32 = jnp.int32

NR = 2048
LOW = -3.0e38


def iota(shape, dim):
    return lax.broadcasted_iota(i32, shape, dim)


def kernel(
    node_h, bag_h, flag_h, bins_h, tgt_h, par_h,
    child_o, best_o, imp_o,
    node_v, bag_v, flag_v, bins_v, tgt_v, par_v,
    bins_b, ev, spread, own, peer, core_r, ring_r, turned, quad_r,
    p16, pchild, amat,
    best_s, best_ra, best_t, best_rb, imp_s, imp_r,
    in_sem, core_ss, core_rs, ring_ss, ring_rs, quad_ss, quad_rs,
    ba_ss, ba_rs, bb_ss, bb_rs, im_ss, im_rs,
):
    z = lax.axis_index("rows_0")
    y = lax.axis_index("rows_1")
    c = lax.axis_index("rows_2")
    t = lax.axis_index("trees")

    def wrap(v, n):
        return jnp.where(v >= n, v - n, v)

    def along_y(off, oc=0):
        return (z, wrap(y + off, 8), 1 - c if oc else c, t)

    def along_z(off):
        return (wrap(z + off, 8), y, c, t)

    def along_x(off):
        return (z, y, c, wrap(t + off, 4))

    def along_p(off):
        return (wrap(z + off * c, 8), wrap(y + off * (1 - c), 8), c, t)

    def along_q(off):
        return (wrap(z + off * (1 - c), 8), wrap(y + off * c, 8), c, t)

    next_p, prev_p = along_p(1), along_p(7)
    qpos = z * (1 - c) + y * c

    small = []
    for i, (src, dst) in enumerate(
        ((node_h, node_v), (bag_h, bag_v), (flag_h, flag_v), (tgt_h, tgt_v), (par_h, par_v))
    ):
        cp = pltpu.make_async_copy(src, dst, in_sem.at[8 + i])
        cp.start()
        small.append(cp)
    loads = []
    for i in range(8):
        cp = pltpu.make_async_copy(
            bins_h.at[pl.ds(256 * i, 256)], bins_v.at[pl.ds(256 * i, 256)], in_sem.at[i]
        )
        cp.start()
        loads.append(cp)

    barrier = pltpu.get_barrier_semaphore()
    greeted = 0
    for oy in range(8):
        for oc in range(2):
            if oy or oc:
                pl.semaphore_signal(barrier, inc=1, device_id=along_y(oy, oc), device_id_type=MESH)
                greeted += 1
    for off in range(1, 8):
        pl.semaphore_signal(barrier, inc=1, device_id=along_z(off), device_id_type=MESH)
        greeted += 1
    for off in range(1, 4):
        pl.semaphore_signal(barrier, inc=1, device_id=along_x(off), device_id_type=MESH)
        greeted += 1

    with jax.named_scope("stats"):
        for cp in small:
            cp.wait()
        flags = flag_v[...]
        row96 = iota((96, 1), 0)
        pair96 = lax.div(row96, 3)
        stat96 = row96 - 3 * pair96
        flag96 = jnp.sum(
            jnp.where(iota((96, 32), 1) == lax.div(iota((96, 32), 0), 3), flags, 0), axis=1, keepdims=True
        )
        chosen = 2 * pair96 + flag96
        for i in range(4):
            part = pl.ds(512 * i, 512)
            node = node_v[:, part]
            wk = bag_v[:, part].astype(f32)
            tgt = tgt_v[:, part]
            first = wk * tgt
            second = first * tgt
            stat = jnp.where(stat96 == 0, wk, jnp.where(stat96 == 1, first, second))
            spread[:, part] = jnp.where(node == chosen, stat, 0.0).astype(bf16)

    with jax.named_scope("cast"):
        for j in range(8):
            loads[j].wait()
            part = pl.ds(256 * j, 256)
            bins_b[part, :] = bins_v[part, :].astype(bf16)

    lane256 = iota((1, 256), 1)
    lane_dd = lax.div(lane256, 128)
    lane_q = lax.rem(lax.div(lane256, 16), 8)
    lane_k = lax.rem(lax.div(lane256, 8), 2)
    lane_b = (4 * lax.rem(lane256, 8)).astype(f32)

    def expander(i, h):
        pos = y * (1 - h) + z * h
        d0 = wrap(pos + 4 + i, 8)
        d1 = wrap(pos + 3 - i, 8)
        d = wrap(d0, 8) * (1 - lane_dd) + d1 * lane_dd
        source = lane_q * (32 - 28 * h) + d * (4 + 28 * h) + 2 * h + lane_k
        return jnp.where(iota((256, 256), 0) == source, 1.0, 0.0).astype(bf16)

    def widen(buf, expand, top):
        for i in (2 * top, 2 * top + 1):
            part = slice(512 * i, 512 * i + 512)
            ev[buf, part, :] = jnp.dot(bins_b[part, :], expand, preferred_element_type=f32).astype(bf16)

    def hot(i, dst, buf, top):
        for bh in (2 * top, 2 * top + 1):
            level = (lane_b + float(bh)).astype(bf16)
            acc = None
            for k in range(8):
                part = slice(256 * k, 256 * k + 256)
                hit = jnp.where(ev[buf, part, :] == level, jnp.ones((), bf16), jnp.zeros((), bf16))
                term = jnp.dot(spread[:, part], hit, preferred_element_type=f32)
                acc = term if acc is None else acc + term
            at = slice(96 * bh, 96 * bh + 96)
            dst[2 * i, at, :] = acc[:, :128]
            dst[2 * i + 1, at, :] = acc[:, 128:]

    def core_copy(i, top):
        part = (pl.ds(2 * i, 2), pl.ds(192 * top, 192))
        return pltpu.make_async_remote_copy(
            src_ref=peer.at[part], dst_ref=core_r.at[part],
            send_sem=core_ss.at[i, top], recv_sem=core_rs.at[i, top],
            device_id=(z, y, 1 - c, t), device_id_type=MESH,
        )

    def merge_core(i, top):
        core_copy(i, top).wait_recv()
        for slot in (2 * i, 2 * i + 1):
            own[slot, 192 * top : 192 * top + 192, :] += core_r[slot, 192 * top : 192 * top + 192, :]

    def ring_copy(way, step, slot, piece):
        rows = pl.ds(96 * piece, 96)
        return pltpu.make_async_remote_copy(
            src_ref=own.at[slot, rows], dst_ref=ring_r.at[way, step, rows],
            send_sem=ring_ss.at[way, step, piece], recv_sem=ring_rs.at[way, step, piece],
            device_id=prev_p if way else next_p, device_id_type=MESH,
        )

    def ring_piece(step, j):
        for way in (0, 1):
            slot = 2 * step if way else 2 * step - 1
            piece = j if way else (j + 2) % 4
            rows = slice(96 * piece, 96 * piece + 96)

            def arrived(way=way, slot=slot, piece=piece, rows=rows):
                ring_copy(way, step - 1, slot, piece).wait_recv()
                own[slot, rows, :] += ring_r[way, step - 1, rows, :]

            if j >= 2:
                arrived()
            else:
                pl.when(step >= 2)(arrived)
            ring_copy(way, step, slot, piece).start()

    widen(0, expander(0, 1 - c), 0)
    widen(0, expander(0, 1 - c), 1)
    with jax.named_scope("barrier_wait"):
        pl.semaphore_wait(barrier, greeted)

    def one_pair(i, carry):
        def ring(j):
            @pl.when(i >= 2)
            def _():
                with jax.named_scope(f"ring{j}"):
                    ring_piece(i - 1, j)

        mine = expander(i, c)
        with jax.named_scope("seg0"):
            widen(1, mine, 0)
            hot(i, peer, 0, 0)
        core_copy(i, 0).start()
        ring(0)
        with jax.named_scope("seg1"):
            widen(1, mine, 1)
            hot(i, peer, 0, 1)
        core_copy(i, 1).start()
        ring(1)
        later = expander(i + 1, 1 - c)
        with jax.named_scope("seg2"):
            widen(0, later, 0)
            hot(i, own, 1, 0)
        with jax.named_scope("merge0"):
            merge_core(i, 0)
        ring(2)
        with jax.named_scope("seg3"):
            widen(0, later, 1)
            hot(i, own, 1, 1)
        with jax.named_scope("merge1"):
            merge_core(i, 1)
        ring(3)

        @pl.when(i == 0)
        def _():
            for piece in (0, 1):
                ring_copy(0, 0, 0, piece).start()
                ring_copy(1, 0, 0, 2 + piece).start()

        return carry

    lax.fori_loop(0, 4, one_pair, 0)
    with jax.named_scope("step3"):
        for j in range(4):
            ring_piece(3, j)

        flag384 = jnp.concatenate([flag96] * 4, axis=0)
        out_lane = iota((1, 768), 1)
        out_bh = lax.div(out_lane, 192)
        out_rest = out_lane - 192 * out_bh
        out_pair = lax.div(out_rest, 6)
        out_six = out_rest - 6 * out_pair
        out_child = lax.div(out_six, 3)
        out_from = 96 * out_bh + 3 * out_pair + (out_six - 3 * out_child)
        for k in range(2):
            for bl in range(8):
                p16[8 * k + bl : 8 * k + bl + 1, :] = par_v[0, k : k + 1, 384 * bl : 384 * bl + 384]
        match = iota((384, 768), 0) == out_from
        is_small = flag384 == out_child
        amat[...] = jnp.where(match, jnp.where(is_small, 1.0, -1.0), 0.0)
        bmat = jnp.where(match, jnp.where(is_small, 0.0, 1.0), 0.0)
        parent = p16[...]
        pchild[...] = jnp.dot(parent, bmat, preferred_element_type=f32, precision=HIGHEST)

    lane = iota((16, 384), 1)
    sub = lax.rem(iota((16, 384), 0), 8)

    def cumulative(x):
        x1 = x + jnp.where(lane >= 96, pltpu.roll(x, 96, 1), 0.0)
        x2 = x1 + jnp.where(lane >= 192, pltpu.roll(x1, 192, 1), 0.0)
        t3 = jnp.where(lane >= 288, x2, 0.0)
        t4 = t3 + pltpu.roll(t3, 96, 1)
        tot = t4 + pltpu.roll(t4, 192, 1)
        before = jnp.where(sub >= 1, pltpu.roll(tot, 1, 0), 0.0)
        for s in (1, 2, 4):
            before = before + jnp.where(sub >= s, pltpu.roll(before, s, 0), 0.0)
        whole = jnp.sum(tot.reshape(2, 8, 384), axis=1, keepdims=True)
        whole = jnp.broadcast_to(whole, (2, 8, 384)).reshape(16, 384)
        return x2 + before, whole

    def gain_of(cb, sb, call, sall):
        gain = sb * sb / (jnp.maximum(cb, 0.0) + 1.0)
        rest = sall - sb
        gain = gain + rest * rest / (jnp.maximum(call - cb, 0.0) + 1.0)
        gain = gain - sall * sall / (jnp.maximum(call, 0.0) + 1.0)
        gain = jnp.where((sub == 7) & (lane >= 288), LOW, gain)
        top = jnp.max(gain.reshape(2, 8, 384), axis=1, keepdims=True)
        top = jnp.broadcast_to(top, (2, 8, 384)).reshape(16, 384)
        top = jnp.maximum(top, pltpu.roll(top, 192, 1))
        return jnp.maximum(top, pltpu.roll(top, 96, 1))

    def left_one(x):
        return pltpu.roll(x, 383, 1)

    with jax.named_scope("parents2"):
        pcum, pall = cumulative(parent)
        psum, psall = left_one(pcum), left_one(pall)

    with jax.named_scope("ring_end"):
        for piece in range(4):
            for way in (0, 1):
                ring_copy(way, 3, 0, piece).wait_recv()
    with jax.named_scope("turn"):
        total = own[7] + ring_r[0, 3] + ring_r[1, 3]
        turned[...] = total.T

    def quad_copy(off):
        to = wrap(qpos + off, 8)
        return pltpu.make_async_remote_copy(
            src_ref=turned.at[pl.ds(pl.multiple_of(16 * to, 16), 16)], dst_ref=quad_r.at[off],
            send_sem=quad_ss.at[off], recv_sem=quad_rs.at[off],
            device_id=along_q(off), device_id_type=MESH,
        )

    far_first = (4, 3, 5, 2, 6, 1, 7)
    for off in far_first:
        quad_copy(off).start()
    with jax.named_scope("quad"):
        hist = turned[pl.ds(pl.multiple_of(16 * qpos, 16), 16), :]
        for off in (1, 7, 2, 6, 3, 5, 4):
            quad_copy(off).wait_recv()
            hist = hist + quad_r[off]

    with jax.named_scope("gains"):
        scum, sall = cumulative(hist)
        ssum, ssall = left_one(scum), left_one(sall)
        gain_s = gain_of(scum, ssum, sall, ssall)
        gain_b = gain_of(pcum - scum, psum - ssum, pall - sall, psall - ssall)
        third = lax.rem(lane, 3)
        both = jnp.where((lane < 96) & (third == 0), gain_s + gain_b, 0.0)
        feat = jnp.sum(both, axis=1, keepdims=True)
        lane8 = iota((8, 128), 1)
        imp_s[...] = jnp.where(lane8 == 0, feat[0:8], jnp.where(lane8 == 1, feat[8:16], 0.0))
        top_s = jnp.maximum(gain_s[0:8], gain_s[8:16])
        top_b = jnp.maximum(gain_b[0:8], gain_b[8:16])
        mixed = jnp.where(third[0:8] == 0, top_s, pltpu.roll(top_b, 1, 1))
        best_s[...] = mixed[:, :128]

    def best_a(oy, oc):
        slot = 2 * oy + oc
        return pltpu.make_async_remote_copy(
            src_ref=best_s, dst_ref=best_ra.at[slot],
            send_sem=ba_ss.at[slot], recv_sem=ba_rs.at[slot],
            device_id=along_y(oy, oc), device_id_type=MESH,
        )

    def best_b(off):
        return pltpu.make_async_remote_copy(
            src_ref=best_t, dst_ref=best_rb.at[off],
            send_sem=bb_ss.at[off], recv_sem=bb_rs.at[off],
            device_id=along_z(off), device_id_type=MESH,
        )

    def imp_copy(off):
        return pltpu.make_async_remote_copy(
            src_ref=imp_s, dst_ref=imp_r.at[off],
            send_sem=im_ss.at[off], recv_sem=im_rs.at[off],
            device_id=along_x(off), device_id_type=MESH,
        )

    others = [(oy, oc) for oy in (4, 3, 5, 2, 6, 1, 7, 0) for oc in (0, 1) if oy or oc]
    for oy, oc in others:
        best_a(oy, oc).start()
    for off in (2, 1, 3):
        imp_copy(off).start()

    with jax.named_scope("kids"):
        kids = pchild[...] + jnp.dot(hist, amat[...], preferred_element_type=f32, precision=HIGHEST)
        for k in range(2):
            for bl in range(8):
                child_o[0, k : k + 1, 768 * bl : 768 * bl + 768] = kids[8 * k + bl : 8 * k + bl + 1, :]

    with jax.named_scope("best_a"):
        top = best_s[...]
        for oy, oc in others:
            best_a(oy, oc).wait_recv()
            top = jnp.maximum(top, best_ra[2 * oy + oc])
    best_t[...] = top
    for off in far_first:
        best_b(off).start()

    with jax.named_scope("pick"):
        flag_col = jnp.sum(jnp.where(iota((32, 32), 0) == iota((32, 32), 1), flags, 0), axis=1, keepdims=True)
        node_lane = iota((32, 64), 1)
        node_flag = jnp.sum(
            jnp.where(lax.div(node_lane, 2) == iota((32, 64), 0), flag_col, 0), axis=0, keepdims=True
        )
        q_lane = iota((1, 64), 1)
        q_pair = lax.div(q_lane, 2)
        taken = 3 * q_pair + jnp.where(q_lane - 2 * q_pair == node_flag, 0, 1)
        pick = jnp.where(iota((128, 64), 0) == taken, 1.0, 0.0)

    with jax.named_scope("imp"):
        share = imp_s[...]
        for off in (1, 3, 2):
            imp_copy(off).wait_recv()
            share = share + imp_r[off]
        imp_o[...] = share[0:1, 0:2] * (1.0 / 256.0)

    with jax.named_scope("best_b"):
        for off in far_first:
            best_b(off).wait_recv()
            top = jnp.maximum(top, best_rb[off])
    best_o[...] = jnp.dot(top, pick, preferred_element_type=f32, precision=HIGHEST)[0:1, :]

    with jax.named_scope("sends"):
        for i in range(4):
            for top in (0, 1):
                core_copy(i, top).wait_send()
        for way in (0, 1):
            for step in range(4):
                for piece in range(4) if step else (2 * way, 2 * way + 1):
                    ring_copy(way, step, 0, piece).wait_send()
        for off in range(1, 8):
            quad_copy(off).wait_send()
            best_b(off).wait_send()
        for oy, oc in others:
            best_a(oy, oc).wait_send()
        for off in range(1, 4):
            imp_copy(off).wait_send()


def hand_over(child, best, imp, child_o, best_o, imp_o):
    child_o[...] = child[...]
    best_o[...] = best[...]
    imp_o[...] = imp[...]


def shards(node_of_row, bag_weight, smaller_side, bins, target, parent_hist):
    any_space = pl.BlockSpec(memory_space=pltpu.HBM)
    vmem = pl.BlockSpec(memory_space=pltpu.VMEM)
    dma = pltpu.SemaphoreType.DMA
    shapes = (
        jax.ShapeDtypeStruct((1, 2, 6144), f32),
        jax.ShapeDtypeStruct((1, 64), f32),
        jax.ShapeDtypeStruct((1, 2), f32),
    )
    results = pl.pallas_call(
        kernel,
        out_shape=shapes,
        in_specs=[any_space] * 6,
        out_specs=(vmem, vmem, vmem),
        scratch_shapes=[
            pltpu.VMEM((1, NR), i32),
            pltpu.VMEM((1, NR), i32),
            pltpu.VMEM((1, 32), i32),
            pltpu.VMEM((NR, 256), i32),
            pltpu.VMEM((1, NR), f32),
            pltpu.VMEM((1, 2, 3072), f32),
            pltpu.VMEM((NR, 256), bf16),
            pltpu.VMEM((2, NR, 256), bf16),
            pltpu.VMEM((96, NR), bf16),
            pltpu.VMEM((8, 384, 128), f32),
            pltpu.VMEM((8, 384, 128), f32),
            pltpu.VMEM((8, 384, 128), f32),
            pltpu.VMEM((2, 4, 384, 128), f32),
            pltpu.VMEM((128, 384), f32),
            pltpu.VMEM((8, 16, 384), f32),
            pltpu.VMEM((16, 384), f32),
            pltpu.VMEM((16, 768), f32),
            pltpu.VMEM((384, 768), f32),
            pltpu.VMEM((8, 128), f32),
            pltpu.VMEM((16, 8, 128), f32),
            pltpu.VMEM((8, 128), f32),
            pltpu.VMEM((8, 8, 128), f32),
            pltpu.VMEM((8, 128), f32),
            pltpu.VMEM((4, 8, 128), f32),
            dma((13,)),
            dma((4, 2)), dma((4, 2)),
            dma((2, 4, 4)), dma((2, 4, 4)),
            dma((8,)), dma((8,)),
            dma((16,)), dma((16,)),
            dma((8,)), dma((8,)),
            dma((4,)), dma((4,)),
        ],
        compiler_params=pltpu.CompilerParams(
            collective_id=0, has_side_effects=True, vmem_limit_bytes=67_043_328
        ),
    )(node_of_row, bag_weight, smaller_side, bins, target.reshape(1, NR), parent_hist)
    child, best, imp = pl.pallas_call(
        hand_over, out_shape=shapes, in_specs=[vmem] * 3, out_specs=(vmem, vmem, vmem)
    )(*results)
    return child, best, imp.reshape(2)


def solution(mesh):
    finer = Mesh(
        mesh.devices.reshape(8, 8, 2, mesh.shape["trees"]), ("rows_0", "rows_1", "rows_2", "trees")
    )
    return jax.shard_map(
        shards,
        mesh=finer,
        in_specs=(
            P("trees", ROWS),
            P("trees", ROWS),
            P("trees", None),
            P(ROWS, None),
            P(ROWS),
            P("trees", ROWS, None),
        ),
        out_specs=(P("trees", ROWS, None), P("trees", None), P(ROWS)),
        check_vma=False,
    )
```
